512 devices in a mesh: row: 64 (over z, y_lo, x), ch: 8 (over y_hi, core).
Axes of the slice: x: 4, y: 8 (y_hi: 4, y_lo: 2; y = y_hi * 2 + y_lo), z: 8, core: 2. Of those that a mesh axis runs over, the one named last changes fastest.
Arguments:
- pair_rep: float32 [1024, 1024, 128], P('row', 'ch'), may hold values from -6 to 6
- residue_mask: int32 [1024], replicated, may hold values 0 or 1
- pair_gain: float32 [2, 128], replicated, may hold values from 0.5 to 1.5
- pair_shift: float32 [2, 128], replicated, may hold values from -3 to 3
- panel_weight: bfloat16 [2, 128, 512], replicated, may hold values from -0.5 to 0.5
- panel_bias: float32 [2, 512], replicated, may hold values from -3 to 3
- gate_weight: bfloat16 [2, 128, 128], replicated, may hold values from -0.5 to 0.5
- gate_bias: float32 [2, 128], replicated, may hold values from -3 to 3
- hidden_gain: float32 [2, 128], replicated, may hold values from 0.5 to 1.5
- hidden_shift: float32 [2, 128], replicated, may hold values from -3 to 3
- output_weight: bfloat16 [2, 128, 128], replicated, may hold values from -0.5 to 0.5
- output_bias: float32 [2, 128], replicated, may hold values from -3 to 3
Outputs:
- updated_pair: float32 [1024, 1024, 128], P('row', 'ch')
The draws below stay inside these ranges and needn't reach their ends.
All inputs are finite; a program needn't handle non-finite values.
Results may differ from the reference program's by a relative error of at most 0.0039.
Values may be sent and summed in bfloat16 or wider, within the bound.
A program may use at most 64 MiB of HBM per device.

```python
import math
import jax
import jax.numpy as jnp
from jax import lax

C = 128
H = 128
N = 1024


def place_ends(array, rng, low, largest):
    spot = [jax.random.randint(jax.random.fold_in(rng, axis), (), 0, length) for axis, length in enumerate(array.shape)]
    widest = array.shape.index(max(array.shape))
    neighbour = spot[:widest] + [(spot[widest] + 1) % array.shape[widest]] + spot[widest + 1:]
    return array.at[tuple(spot)].set(low).at[tuple(neighbour)].set(largest)


def levels(own_key, extent, cuts, smallest, top_value):
    factor_of, own = 1.0, jax.random.fold_in(own_key, 6)
    for axis_at, parts in cuts:
        steps = jnp.exp(jax.random.uniform(jax.random.fold_in(own, axis_at), (parts,), jnp.float32, smallest / len(cuts), top_value / len(cuts)))
        factor_of = factor_of * jnp.repeat(steps, extent[axis_at] // parts).reshape([-1 if axis == axis_at else 1 for axis in range(len(extent))])
    return factor_of


def noise(stream_key, dims, scale, most, cuts=(), kind=jnp.bfloat16):
    array = jax.random.normal(stream_key, dims, jnp.float32) * scale
    if len(cuts) > 0:
        array = levels(stream_key, dims, cuts, -0.22, 0.18) * array
    return jnp.clip(array, min=-most, max=most).astype(kind)


def setup_inputs(seed: int = 0) -> dict:
    key_of = jax.random.split(jax.random.key(seed), 13)
    pair_rep = noise(key_of[0], (N, N, C), 1.0, 6.0, ((0, 64), (1, 8)), jnp.float32)
    residue_mask = place_ends((jax.random.randint(key_of[1], (N,), 0, 8) < 7).astype(jnp.int32), jax.random.fold_in(key_of[1], 1), 0, 1)
    pair_gain = jnp.clip(jax.random.uniform(key_of[2], (2, C), jnp.float32, 0.5, 1.5), 0.5, 1.5)
    pair_shift = noise(key_of[3], (2, C), 0.5, 3.0, (), jnp.float32)
    panel_weight = noise(key_of[4], (2, C, 4 * H), C ** -0.5, 0.5)
    panel_bias = noise(key_of[5], (2, 4 * H), 0.5, 3.0, (), jnp.float32)
    gate_weight = noise(key_of[6], (2, C, C), C ** -0.5, 0.5)
    gate_bias = noise(key_of[7], (2, C), 0.5, 3.0, (), jnp.float32)
    hidden_gain = jnp.clip(jax.random.uniform(key_of[8], (2, H), jnp.float32, 0.5, 1.5), 0.5, 1.5)
    hidden_shift = noise(key_of[9], (2, H), 0.5, 3.0, (), jnp.float32)
    output_weight = noise(key_of[10], (2, H, C), H ** -0.5, 0.5)
    output_bias = noise(key_of[11], (2, C), 0.5, 3.0, (), jnp.float32)
    return dict(pair_rep=pair_rep, residue_mask=residue_mask, pair_gain=pair_gain, pair_shift=pair_shift, panel_weight=panel_weight, panel_bias=panel_bias, gate_weight=gate_weight, gate_bias=gate_bias, hidden_gain=hidden_gain, hidden_shift=hidden_shift, output_weight=output_weight, output_bias=output_bias)


PAIR_EPSILON = 1e-05
HIDDEN_EPSILON = 1.0

def layer_norm(values, gain_value, shift_value, along, epsilon):
    center = lax.optimization_barrier(jnp.mean(values, axis=along, keepdims=True))
    offset = values - center
    spread = lax.optimization_barrier(jnp.mean(offset * offset, axis=along, keepdims=True))
    return offset * lax.rsqrt(spread + epsilon) * gain_value + shift_value

def update(current, cell_mask, section_index, pair_gain, pair_shift, panel_weight, panel_bias, gate_weight, gate_bias, hidden_gain, hidden_shift, output_weight, output_bias):
    normed = layer_norm(current, pair_gain[section_index], pair_shift[section_index], -1, PAIR_EPSILON).astype(jnp.bfloat16)
    flattened = normed.reshape(N * N, C)
    weight = panel_weight[section_index]
    biases = panel_bias[section_index]

    def column(which_one):
        result = jnp.dot(flattened, weight[:, which_one * H:(which_one + 1) * H], preferred_element_type=jnp.float32)
        return (result + biases[which_one * H:(which_one + 1) * H]).reshape(N, N, H)
    left_panel = (cell_mask[:, :, None] * jax.nn.sigmoid(column(0)) * column(1)).astype(jnp.bfloat16)
    right_panel = (cell_mask[:, :, None] * jax.nn.sigmoid(column(2)) * column(3)).astype(jnp.bfloat16)
    gate_value = jax.nn.sigmoid(jnp.dot(flattened, gate_weight[section_index], preferred_element_type=jnp.float32) + gate_bias[section_index]).reshape(N, N, C)
    if section_index == 1:
        left_panel = jnp.transpose(left_panel, (1, 0, 2))
        right_panel = jnp.transpose(right_panel, (1, 0, 2))
    left_hidden = jnp.transpose(left_panel, (2, 0, 1)).astype(jnp.float32)
    right_hidden = jnp.transpose(right_panel, (2, 0, 1)).astype(jnp.float32)
    block_rows = math.gcd(N, 128)
    block_count = N // block_rows
    out_weight = output_weight[section_index].astype(jnp.float32)

    def one_block(block_index):
        row_start = block_index * block_rows
        left_rows = lax.dynamic_slice_in_dim(left_hidden, row_start, block_rows, 1)
        products = jnp.einsum('hik,hjk->hij', left_rows, right_hidden, precision=lax.Precision.HIGHEST)
        normed_hidden = layer_norm(products, hidden_gain[section_index][:, None, None], hidden_shift[section_index][:, None, None], 0, HIDDEN_EPSILON).astype(jnp.bfloat16)
        projected = jnp.einsum('hij,hc->ijc', normed_hidden.astype(jnp.float32), out_weight, precision=lax.Precision.HIGHEST)
        gate_rows = lax.dynamic_slice_in_dim(gate_value, row_start, block_rows, 0)
        return gate_rows * (projected + output_bias[section_index])
    updates = lax.map(one_block, jnp.arange(block_count, dtype=jnp.int32))
    return current + updates.reshape(N, N, C)

def reference(pair_rep, residue_mask, pair_gain, pair_shift, panel_weight, panel_bias, gate_weight, gate_bias, hidden_gain, hidden_shift, output_weight, output_bias):
    residue_float = residue_mask.astype(jnp.float32)
    cell_mask = residue_float[:, None] * residue_float[None, :]
    current = pair_rep
    for section_index in range(2):
        current = update(current, cell_mask, section_index, pair_gain, pair_shift, panel_weight, panel_bias, gate_weight, gate_bias, hidden_gain, hidden_shift, output_weight, output_bias)
    return current
```

```python
import functools

import jax
import jax.numpy as jnp
from jax import lax
from jax.experimental import pallas as pl
from jax.experimental.pallas import tpu as pltpu
from jax.sharding import PartitionSpec as P

PAIR_EPSILON = 1e-05
HIDDEN_EPSILON = 1.0
MESH = pl.DeviceIdType.MESH
HIDDEN = 128
TILE = 16
LANE = 128


def layer_norm(values, gain_value, shift_value, along, epsilon):
    center = jnp.mean(values, axis=along, keepdims=True)
    offset = values - center
    spread = jnp.mean(offset * offset, axis=along, keepdims=True)
    return offset * lax.rsqrt(spread + epsilon) * gain_value + shift_value


def shuffled(t):
    dz = (5 * t) % 8
    dy = (t // 8 + 3 * t) % 8
    return dz, dy, t // 64


def triangle_kernel(section, left_ref, right_ref, out_ref, abuf, bbuf, xbuf, xrecv, send_sem, recv_sem):
    row = lax.axis_index("row")
    ch = lax.axis_index("ch")
    z, y_lo, x = row // 8, (row // 4) % 2, row % 4
    y_hi, core = ch // 2, ch % 2
    y = y_hi * 2 + y_lo
    x_hi, x_lo = x // 2, x % 2
    hx = x + x_hi * (3 - 2 * x)
    half = x_hi
    own_h = z * 16 + y * 2 + hx

    if section == 0:
        a_half, a_core = x_hi, core
        b_half, b_core = x_hi, z % 2
        a_slot = abuf.at[
            core, pl.ds((z * 4 + y_lo * 2 + x_lo) * TILE, TILE), pl.ds(y_hi * LANE, LANE)
        ]
        b_slot = bbuf.at[
            core, z // 2, y_lo, x_hi, pl.ds(x_lo * TILE, TILE), pl.ds(y_hi * LANE, LANE)
        ]
        a_self = None
        b_self = core == z % 2
    else:
        a_half, a_core = y_hi // 2, core
        b_half, b_core = x_hi, core
        a_slot = abuf.at[core, pl.ds(row * TILE, TILE), pl.ds((y_hi % 2) * LANE, LANE)]
        b_slot = bbuf.at[
            z // 4, z % 4, y_lo, x_hi, pl.ds(x_lo * TILE, TILE), pl.ds(y_hi * LANE, LANE)
        ]
        a_self = y_hi // 2 == x_hi
        b_self = None

    def target(t, to_half, to_core):
        dz, dy, dx = shuffled(t)
        z_t, y_t, hx_t = (z + dz) % 8, (y + dy) % 8, (hx + dx) % 2
        x_t = hx_t + to_half * (3 - 2 * hx_t)
        there = {"row": z_t * 8 + (y_t % 2) * 4 + x_t, "ch": (y_t // 2) * 2 + to_core}
        return z_t * 16 + y_t * 2 + hx_t, there

    def remote(src, dst, sent, got, there):
        return pltpu.make_async_remote_copy(
            src_ref=src,
            dst_ref=dst,
            send_sem=send_sem.at[sent],
            recv_sem=recv_sem.at[got],
            device_id=there,
            device_id_type=MESH,
        )

    def first(src, dst, sent, got, there, to_self):
        local = pltpu.make_async_copy(src, dst, recv_sem.at[got])
        if to_self is None:
            local.start()
        else:
            pl.when(to_self)(local.start)
            pl.when(jnp.logical_not(to_self))(remote(src, dst, sent, got, there).start)

    def first_done(src, sent, to_self):
        if to_self is not None:
            pl.when(jnp.logical_not(to_self))(
                pltpu.make_async_copy(src, src, send_sem.at[sent]).wait
            )

    def panel_sends(ref, slot, to_half, to_core, sent, got, to_self):
        h_0, there_0 = target(0, to_half, to_core)
        first(ref.at[h_0], slot, sent + 1, got, there_0, to_self)

        def body(t, carry):
            h_t, there = target(t, to_half, to_core)
            remote(ref.at[h_t], slot, sent, got, there).start()
            return carry

        lax.fori_loop(1, HIDDEN, body, 0)

    def got_all(got):
        pltpu.make_async_copy(left_ref, left_ref, recv_sem.at[got]).wait()

    def sent_all(sent, to_self):
        rest = left_ref.at[pl.ds(0, HIDDEN - 1)]
        pltpu.make_async_copy(rest, rest, send_sem.at[sent]).wait()
        first_done(left_ref.at[0], sent + 1, to_self)

    panel_sends(right_ref, b_slot, b_half, b_core, 0, 0, b_self)
    panel_sends(left_ref, a_slot, a_half, a_core, 2, 1, a_self)

    got_all(0)
    partner = {"row": row + 3 - 2 * x, "ch": ch}
    for outer in range(2):
        for inner in range(4):
            for low in range(2):
                block = bbuf.at[outer, inner, low, half] if section == 0 else bbuf.at[outer, inner, low, half]
                remote(block, block, 4, 2, partner).start()
    got_all(1)
    sibling = {"row": row, "ch": ch + 1 - 2 * core}
    remote(abuf.at[core], abuf.at[core], 5, 3, sibling).start()
    got_all(2)
    got_all(3)

    if section == 0:
        products = None
        for part in range(2):
            right = bbuf[part].reshape(512, 512)
            term = lax.dot_general(
                abuf[part], right, (((1,), (1,)), ((), ())), preferred_element_type=jnp.float32
            )
            products = term if products is None else products + term
        xbuf[...] = products.astype(jnp.bfloat16)
    else:
        right = bbuf[...].reshape(1024, 512)
        for part in range(2):
            term = lax.dot_general(
                abuf[part], right, (((0,), (0,)), ((), ())), preferred_element_type=jnp.float32
            )
            xbuf[pl.ds(part * 256, 256), :] = term.astype(jnp.bfloat16)

    def cell(t):
        dz, dy, dx = shuffled(t)
        y_t = (y + dy) % 8
        if section == 0:
            z_t, low_t = (z + dz) % 8, (x_lo + dx) % 2
            block = z_t * 4 + (y_t % 2) * 2 + low_t
            row_t = z_t * 8 + (y_t % 2) * 4 + half * 2 + low_t
        else:
            q_t = (z + dz % 4) % 4
            x_t = (x + (dz // 4) * 2 + dx) % 4
            block = (q_t % 2) * 16 + (q_t // 2) * 8 + (y_t % 2) * 4 + x_t
            row_t = half * 32 + q_t * 8 + (y_t % 2) * 4 + x_t
        src = xbuf.at[pl.ds(block * TILE, TILE), pl.ds((y_t // 2) * LANE, LANE)]
        return src, {"row": row_t, "ch": (y_t // 2) * 2 + core}

    x_self = None if section == 0 else z // 4 == half
    src_0, there_0 = cell(0)
    first(src_0, xrecv.at[own_h], 7, 4, there_0, x_self)

    def body(t, carry):
        src, there = cell(t)
        remote(src, xrecv.at[own_h], 6, 4, there).start()
        return carry

    lax.fori_loop(1, HIDDEN, body, 0)
    sent_all(0, b_self)
    sent_all(2, a_self)
    pltpu.make_async_copy(left_ref, left_ref, send_sem.at[4]).wait()
    pltpu.make_async_copy(left_ref, left_ref, send_sem.at[5]).wait()
    got_all(4)
    out_ref[...] = xrecv[...]
    sent_all(6, x_self)


def triangle(section, left_panel, right_panel):
    abuf = (2, 512, 512) if section == 0 else (2, 1024, 256)
    return pl.pallas_call(
        functools.partial(triangle_kernel, section),
        out_shape=jax.ShapeDtypeStruct((HIDDEN, TILE, LANE), jnp.bfloat16),
        in_specs=[pl.BlockSpec(memory_space=pltpu.VMEM)] * 2,
        out_specs=pl.BlockSpec(memory_space=pltpu.VMEM),
        scratch_shapes=[
            pltpu.VMEM(abuf, jnp.bfloat16),
            pltpu.VMEM((2, 4, 2, 2, 32, 512), jnp.bfloat16),
            pltpu.VMEM((512, 512), jnp.bfloat16),
            pltpu.VMEM((HIDDEN, TILE, LANE), jnp.bfloat16),
            pltpu.SemaphoreType.DMA((8,)),
            pltpu.SemaphoreType.DMA((5,)),
        ],
        compiler_params=pltpu.CompilerParams(has_side_effects=True),
        name=f"triangle_{section}",
    )(left_panel, right_panel)


def project(
    current,
    cell_mask,
    section_index,
    pair_gain,
    pair_shift,
    panel_weight,
    panel_bias,
    gate_weight,
    gate_bias,
):
    normed = layer_norm(
        current, pair_gain[section_index], pair_shift[section_index], 2, PAIR_EPSILON
    ).astype(jnp.bfloat16)
    features = jnp.einsum(
        "rjc,cf->frj", normed, panel_weight[section_index], preferred_element_type=jnp.float32
    )
    features = features + panel_bias[section_index][:, None, None]
    left_panel = (
        cell_mask * jax.nn.sigmoid(features[:HIDDEN]) * features[HIDDEN : 2 * HIDDEN]
    ).astype(jnp.bfloat16)
    right_panel = (
        cell_mask
        * jax.nn.sigmoid(features[2 * HIDDEN : 3 * HIDDEN])
        * features[3 * HIDDEN :]
    ).astype(jnp.bfloat16)
    gate_value = jax.nn.sigmoid(
        jnp.einsum(
            "rjc,cd->rjd", normed, gate_weight[section_index], preferred_element_type=jnp.float32
        )
        + gate_bias[section_index]
    )
    return (left_panel, right_panel, gate_value)


def local(
    pair_rep,
    residue_mask,
    pair_gain,
    pair_shift,
    panel_weight,
    panel_bias,
    gate_weight,
    gate_bias,
    hidden_gain,
    hidden_shift,
    output_weight,
    output_bias,
):
    row_count = pair_rep.shape[0]
    col_count = pair_rep.shape[1]
    row_index = lax.axis_index("row")
    col_index = lax.axis_index("ch")
    residue_float = residue_mask.astype(jnp.float32)
    row_mask = lax.dynamic_slice_in_dim(residue_float, row_index * row_count, row_count)
    col_mask = lax.dynamic_slice_in_dim(residue_float, col_index * col_count, col_count)
    cell_mask = row_mask[:, None] * col_mask[None, :]
    current = pair_rep
    for section_index in range(2):
        left_panel, right_panel, gate_value = project(
            current,
            cell_mask,
            section_index,
            pair_gain,
            pair_shift,
            panel_weight,
            panel_bias,
            gate_weight,
            gate_bias,
        )
        gathered = triangle(section_index, left_panel, right_panel).astype(jnp.float32)
        normed = layer_norm(
            gathered,
            hidden_gain[section_index][:, None, None],
            hidden_shift[section_index][:, None, None],
            0,
            HIDDEN_EPSILON,
        ).astype(jnp.bfloat16)
        projected = jnp.einsum(
            "hrj,hc->rjc", normed, output_weight[section_index], preferred_element_type=jnp.float32
        )
        current = current + gate_value * (projected + output_bias[section_index])
    return current


def solution(mesh):
    return jax.shard_map(
        local,
        mesh=mesh,
        in_specs=(P("row", "ch", None), P(), P(), P(), P(), P(), P(), P(), P(), P(), P(), P()),
        out_specs=P("row", "ch", None),
        check_vma=False,
    )
```

```python
import functools

import jax
import jax.numpy as jnp
from jax import lax
from jax.experimental import pallas as pl
from jax.experimental.pallas import tpu as pltpu
from jax.sharding import PartitionSpec as P

PAIR_EPSILON = 1e-05
HIDDEN_EPSILON = 1.0
MESH = pl.DeviceIdType.MESH
HIDDEN = 128
TILE = 16
LANE = 128
DEVICES = 512
CHANNELS = 8


def sigmoid(values):
    return 0.5 * jnp.tanh(0.5 * values) + 0.5


def shuffled(t):
    dz = (5 * t) % 8
    dy = (t // 8 + 3 * t) % 8
    return dz, dy, t // 64


def evoformer_kernel(
    row_mask_ref,
    hidden_gain_ref,
    hidden_shift_ref,
    pair_ref,
    col_mask_ref,
    pair_gain_ref,
    pair_shift_ref,
    panel_weight_ref,
    panel_bias_ref,
    gate_weight_ref,
    gate_bias_ref,
    output_weight_ref,
    output_bias_ref,
    out_ref,
    weight_buf,
    bias_buf,
    normed_buf,
    gate_buf,
    wide_buf,
    left_send,
    right_send,
    abuf_0,
    abuf_1,
    bbuf_0,
    bbuf_1,
    xbuf,
    xrecv,
    send_sem,
    recv_sem,
):
    row = lax.axis_index("row")
    ch = lax.axis_index("ch")
    z, y_lo, x = row // 8, (row // 4) % 2, row % 4
    y_hi, core = ch // 2, ch % 2
    y = y_hi * 2 + y_lo
    x_hi, x_lo = x // 2, x % 2
    hx = x + x_hi * (3 - 2 * x)
    half = x_hi
    own_h = z * 16 + y * 2 + hx

    barrier = pltpu.get_barrier_semaphore()
    me = row * CHANNELS + ch

    def greet(t, carry):
        other = (me + t) % DEVICES
        there = {"row": other // CHANNELS, "ch": other % CHANNELS}
        pl.semaphore_signal(barrier, inc=1, device_id=there, device_id_type=MESH)
        return carry

    lax.fori_loop(1, DEVICES, greet, 0)

    col_mask = col_mask_ref[pl.ds(ch, 1), :].astype(jnp.float32)

    def prepare(section):
        weight = panel_weight_ref[section].astype(jnp.float32)
        weight_buf[section] = weight.T.astype(jnp.bfloat16)
        bias = panel_bias_ref[pl.ds(section, 1), :]
        bias_buf[section] = jnp.broadcast_to(bias, (LANE, 4 * HIDDEN)).T

    def normalize(section, source):
        gain = pair_gain_ref[pl.ds(section, 1), :]
        shift = pair_shift_ref[pl.ds(section, 1), :]

        def body(r, carry):
            values = source[r]
            offset = values - jnp.mean(values, axis=-1, keepdims=True)
            spread = jnp.mean(offset * offset, axis=-1, keepdims=True)
            normed = offset * lax.rsqrt(spread + PAIR_EPSILON) * gain + shift
            normed_buf[r] = normed.astype(jnp.bfloat16)
            return carry

        lax.fori_loop(0, TILE, body, 0, unroll=4)

    def panel(section, base, send_ref):
        def body(r, carry):
            features = lax.dot_general(
                weight_buf[section, pl.ds(base, 2 * HIDDEN)],
                normed_buf[r],
                (((1,), (1,)), ((), ())),
                preferred_element_type=jnp.float32,
            )
            features = features + bias_buf[section, pl.ds(base, 2 * HIDDEN)]
            mask = col_mask * row_mask_ref[row * TILE + r].astype(jnp.float32)
            values = mask * sigmoid(features[:HIDDEN]) * features[HIDDEN:]
            wide_buf[pl.ds(r, HIDDEN, stride=TILE), :] = values
            return carry

        lax.fori_loop(0, TILE, body, 0, unroll=4)

        def pack(i, carry):
            part = wide_buf[pl.ds(i * 16 * TILE, 16 * TILE), :]
            send_ref[pl.ds(i * 16, 16)] = part.reshape(16, TILE, LANE).astype(jnp.bfloat16)
            return carry

        lax.fori_loop(0, 8, pack, 0)

    def gate(section):
        def body(r, carry):
            values = jnp.dot(
                normed_buf[r], gate_weight_ref[section], preferred_element_type=jnp.float32
            )
            gate_buf[r] = sigmoid(values + gate_bias_ref[pl.ds(section, 1), :])
            return carry

        lax.fori_loop(0, TILE, body, 0, unroll=4)

    def finish(section, source):
        got = xrecv.at[section]

        def total(i, carry):
            return carry + jnp.sum(got[pl.ds(i * 16, 16)].astype(jnp.float32), axis=0)

        zero = jnp.zeros((TILE, LANE), jnp.float32)
        center = lax.fori_loop(0, 8, total, zero) * (1.0 / HIDDEN)

        def squares(i, carry):
            offset = got[pl.ds(i * 16, 16)].astype(jnp.float32) - center
            return carry + jnp.sum(offset * offset, axis=0)

        spread = lax.fori_loop(0, 8, squares, zero) * (1.0 / HIDDEN)
        scale = lax.rsqrt(spread + HIDDEN_EPSILON)

        def rescale(h, carry):
            offset = got[h].astype(jnp.float32) - center
            values = offset * scale * hidden_gain_ref[section, h] + hidden_shift_ref[section, h]
            wide_buf[pl.ds(pl.multiple_of(h * TILE, TILE), TILE), :] = values
            return carry

        lax.fori_loop(0, HIDDEN, rescale, 0, unroll=8)

        def body(r, carry):
            normed = wide_buf[pl.ds(r, HIDDEN, stride=TILE), :].astype(jnp.bfloat16)
            projected = lax.dot_general(
                normed,
                output_weight_ref[section],
                (((0,), (0,)), ((), ())),
                preferred_element_type=jnp.float32,
            )
            projected = projected + output_bias_ref[pl.ds(section, 1), :]
            out_ref[r] = source[r] + gate_buf[r] * projected
            return carry

        lax.fori_loop(0, TILE, body, 0, unroll=4)

    def remote(src, dst, sent, got, there):
        return pltpu.make_async_remote_copy(
            src_ref=src,
            dst_ref=dst,
            send_sem=send_sem.at[sent],
            recv_sem=recv_sem.at[got],
            device_id=there,
            device_id_type=MESH,
        )

    def first(src, dst, sent, got, there, to_self):
        local = pltpu.make_async_copy(src, dst, recv_sem.at[got])
        if to_self is None:
            local.start()
        else:
            pl.when(to_self)(local.start)
            pl.when(jnp.logical_not(to_self))(remote(src, dst, sent, got, there).start)

    def got_all(got):
        pltpu.make_async_copy(left_send, left_send, recv_sem.at[got]).wait()

    def sent_all(sent):
        pltpu.make_async_copy(left_send, left_send, send_sem.at[sent]).wait()

    def sent_rest(sent, to_self):
        rest = left_send.at[pl.ds(0, HIDDEN - 1)]
        pltpu.make_async_copy(rest, rest, send_sem.at[sent]).wait()
        if to_self is not None:
            one = left_send.at[0]
            pl.when(jnp.logical_not(to_self))(
                pltpu.make_async_copy(one, one, send_sem.at[sent + 1]).wait
            )

    def target(t, to_half, to_core):
        dz, dy, dx = shuffled(t)
        z_t, y_t, hx_t = (z + dz) % 8, (y + dy) % 8, (hx + dx) % 2
        x_t = hx_t + to_half * (3 - 2 * hx_t)
        there = {"row": z_t * 8 + (y_t % 2) * 4 + x_t, "ch": (y_t // 2) * 2 + to_core}
        return z_t * 16 + y_t * 2 + hx_t, there

    def panel_sends(ref, slot, to_half, to_core, sent, got, to_self):
        h_0, there_0 = target(0, to_half, to_core)
        first(ref.at[h_0], slot, sent + 1, got, there_0, to_self)

        def body(t, carry):
            h_t, there = target(t, to_half, to_core)
            remote(ref.at[h_t], slot, sent, got, there).start()
            return carry

        lax.fori_loop(1, HIDDEN, body, 0)

    partner = {"row": row + 3 - 2 * x, "ch": ch}
    sibling = {"row": row, "ch": ch + 1 - 2 * core}

    def update(section, source):
        abuf = abuf_0 if section == 0 else abuf_1
        bbuf = bbuf_0 if section == 0 else bbuf_1
        sends, gots = 8 * section, 5 * section
        lanes = pl.ds(x_lo * TILE, TILE), pl.ds(y_hi * LANE, LANE)
        if section == 0:
            a_half, a_core = x_hi, core
            b_half, b_core = x_hi, z % 2
            a_slot = abuf.at[core, pl.ds((z * 4 + y_lo * 2 + x_lo) * TILE, TILE), lanes[1]]
            b_slot = bbuf.at[core, z // 2, y_lo, x_hi, lanes[0], lanes[1]]
            a_self, b_self = None, core == z % 2
        else:
            a_half, a_core = y_hi // 2, core
            b_half, b_core = x_hi, core
            a_slot = abuf.at[core, pl.ds(row * TILE, TILE), pl.ds((y_hi % 2) * LANE, LANE)]
            b_slot = bbuf.at[z // 4, z % 4, y_lo, x_hi, lanes[0], lanes[1]]
            a_self, b_self = y_hi // 2 == x_hi, None

        normalize(section, source)
        panel(section, 2 * HIDDEN, right_send)
        if section == 0:
            pl.semaphore_wait(barrier, DEVICES - 1)
        panel_sends(right_send, b_slot, b_half, b_core, sends, gots, b_self)
        panel(section, 0, left_send)
        panel_sends(left_send, a_slot, a_half, a_core, sends + 2, gots + 1, a_self)
        gate(section)

        got_all(gots)
        for outer in range(2):
            for inner in range(4):
                for low in range(2):
                    block = bbuf.at[outer, inner, low, half]
                    remote(block, block, sends + 4, gots + 2, partner).start()
        got_all(gots + 1)
        remote(abuf.at[core], abuf.at[core], sends + 5, gots + 3, sibling).start()
        got_all(gots + 2)
        got_all(gots + 3)

        if section == 0:
            products = None
            for part in range(2):
                term = lax.dot_general(
                    abuf[part],
                    bbuf[part].reshape(512, 512),
                    (((1,), (1,)), ((), ())),
                    preferred_element_type=jnp.float32,
                )
                products = term if products is None else products + term
            xbuf[section] = products.astype(jnp.bfloat16)
        else:
            right = bbuf[...].reshape(1024, 512)
            for part in range(2):
                term = lax.dot_general(
                    abuf[part], right, (((0,), (0,)), ((), ())), preferred_element_type=jnp.float32
                )
                xbuf[section, pl.ds(part * 256, 256), :] = term.astype(jnp.bfloat16)

        def cell(t):
            dz, dy, dx = shuffled(t)
            y_t = (y + dy) % 8
            if section == 0:
                z_t, low_t = (z + dz) % 8, (x_lo + dx) % 2
                block = z_t * 4 + (y_t % 2) * 2 + low_t
                row_t = z_t * 8 + (y_t % 2) * 4 + half * 2 + low_t
            else:
                q_t = (z + dz % 4) % 4
                x_t = (x + (dz // 4) * 2 + dx) % 4
                block = (q_t % 2) * 16 + (q_t // 2) * 8 + (y_t % 2) * 4 + x_t
                row_t = half * 32 + q_t * 8 + (y_t % 2) * 4 + x_t
            src = xbuf.at[section, pl.ds(block * TILE, TILE), pl.ds((y_t // 2) * LANE, LANE)]
            return src, {"row": row_t, "ch": (y_t // 2) * 2 + core}

        x_self = None if section == 0 else z // 4 == half
        x_slot = xrecv.at[section, own_h]
        src_0, there_0 = cell(0)
        first(src_0, x_slot, sends + 7, gots + 4, there_0, x_self)

        def body(t, carry):
            src, there = cell(t)
            remote(src, x_slot, sends + 6, gots + 4, there).start()
            return carry

        lax.fori_loop(1, HIDDEN, body, 0)
        sent_rest(sends, b_self)
        sent_rest(sends + 2, a_self)
        sent_all(sends + 4)
        sent_all(sends + 5)
        got_all(gots + 4)
        finish(section, source)
        sent_rest(sends + 6, x_self)

    prepare(0)
    prepare(1)
    update(0, pair_ref)
    update(1, out_ref)


def local(
    pair_rep,
    residue_mask,
    pair_gain,
    pair_shift,
    panel_weight,
    panel_bias,
    gate_weight,
    gate_bias,
    hidden_gain,
    hidden_shift,
    output_weight,
    output_bias,
):
    smem = pl.BlockSpec(memory_space=pltpu.SMEM)
    vmem = pl.BlockSpec(memory_space=pltpu.VMEM)
    half = jnp.bfloat16
    return pl.pallas_call(
        evoformer_kernel,
        out_shape=jax.ShapeDtypeStruct(pair_rep.shape, jnp.float32),
        in_specs=[smem] * 3 + [vmem] * 10,
        out_specs=vmem,
        scratch_shapes=[
            pltpu.VMEM((2, 4 * HIDDEN, LANE), half),
            pltpu.VMEM((2, 4 * HIDDEN, LANE), jnp.float32),
            pltpu.VMEM((TILE, LANE, LANE), half),
            pltpu.VMEM((TILE, LANE, LANE), jnp.float32),
            pltpu.VMEM((HIDDEN * TILE, LANE), jnp.float32),
            pltpu.VMEM((HIDDEN, TILE, LANE), half),
            pltpu.VMEM((HIDDEN, TILE, LANE), half),
            pltpu.VMEM((2, 512, 512), half),
            pltpu.VMEM((2, 1024, 256), half),
            pltpu.VMEM((2, 4, 2, 2, 32, 512), half),
            pltpu.VMEM((2, 4, 2, 2, 32, 512), half),
            pltpu.VMEM((2, 512, 512), half),
            pltpu.VMEM((2, HIDDEN, TILE, LANE), half),
            pltpu.SemaphoreType.DMA((16,)),
            pltpu.SemaphoreType.DMA((10,)),
        ],
        compiler_params=pltpu.CompilerParams(collective_id=0, has_side_effects=True),
        name="evoformer",
    )(
        residue_mask,
        hidden_gain,
        hidden_shift,
        pair_rep,
        residue_mask.reshape(CHANNELS, LANE),
        pair_gain,
        pair_shift,
        panel_weight,
        panel_bias,
        gate_weight,
        gate_bias,
        output_weight,
        output_bias,
    )


def solution(mesh):
    return jax.shard_map(
        local,
        mesh=mesh,
        in_specs=(P("row", "ch", None), P(), P(), P(), P(), P(), P(), P(), P(), P(), P(), P()),
        out_specs=P("row", "ch", None),
        check_vma=False,
    )
```

```python
import functools

import jax
import jax.numpy as jnp
from jax import lax
from jax.experimental import pallas as pl
from jax.experimental.pallas import tpu as pltpu
from jax.sharding import PartitionSpec as P

PAIR_EPSILON = 1e-05
HIDDEN_EPSILON = 1.0
MESH = pl.DeviceIdType.MESH
HIDDEN = 128
TILE = 16
LANE = 128
CHANNELS = 8


def sigmoid(values):
    return 0.5 * jnp.tanh(0.5 * values) + 0.5


def shuffled(t):
    dz = (5 * t) % 8
    dy = (t // 8 + 3 * t) % 8
    return dz, dy, t // 64


def evoformer_kernel(
    row_mask_ref,
    hidden_gain_ref,
    hidden_shift_ref,
    pair_ref,
    col_mask_ref,
    pair_gain_ref,
    pair_shift_ref,
    panel_weight_ref,
    panel_bias_ref,
    gate_weight_ref,
    gate_bias_ref,
    output_weight_ref,
    output_bias_ref,
    out_ref,
    pair_buf,
    weight_buf,
    bias_buf,
    normed_buf,
    gate_buf,
    wide_buf,
    left_send,
    right_send,
    pair_bufs,
    core_bufs,
    xbuf,
    xrecv,
    send_sem,
    recv_sem,
    io_sem,
    ready_sem,
):
    row = lax.axis_index("row")
    ch = lax.axis_index("ch")
    z, y_lo, x = row // 8, (row // 4) % 2, row % 4
    y_hi, core = ch // 2, ch % 2
    y = y_hi * 2 + y_lo
    x_hi, x_lo = x // 2, x % 2
    hx = x + x_hi * (3 - 2 * x)
    half = x_hi
    own_h = z * 16 + y * 2 + hx

    barrier = pltpu.get_barrier_semaphore()
    load = pltpu.make_async_copy(pair_ref, pair_buf, io_sem.at[0])
    load.start()

    def column(t):
        spot = (y_lo * CHANNELS + ch + t) % 16
        return {"row": z * 8 + (spot // CHANNELS) * 4 + x, "ch": spot % CHANNELS}

    def plane(t):
        spot = (z * 4 + x + t) % 32
        return {"row": (spot // 4) * 8 + y_lo * 4 + spot % 4, "ch": ch}

    def signals(sem, group, count):
        def body(t, carry):
            pl.semaphore_signal(sem, inc=1, device_id=group(t), device_id_type=MESH)
            return carry

        lax.fori_loop(1, count, body, 0)

    signals(barrier, plane, 32)
    signals(barrier, column, 16)

    col_mask = col_mask_ref[pl.ds(ch, 1), :].astype(jnp.float32)

    def prepare(section):
        weight = panel_weight_ref[section].astype(jnp.float32)
        weight_buf[section] = weight.T.astype(jnp.bfloat16)
        bias = panel_bias_ref[pl.ds(section, 1), :]
        bias_buf[section] = jnp.broadcast_to(bias, (LANE, 4 * HIDDEN)).T

    def normalize(section):
        gain = pair_gain_ref[pl.ds(section, 1), :]
        shift = pair_shift_ref[pl.ds(section, 1), :]

        def body(r, carry):
            values = pair_buf[r]
            offset = values - jnp.mean(values, axis=-1, keepdims=True)
            spread = jnp.mean(offset * offset, axis=-1, keepdims=True)
            normed = offset * lax.rsqrt(spread + PAIR_EPSILON) * gain + shift
            normed_buf[r] = normed.astype(jnp.bfloat16)
            return carry

        lax.fori_loop(0, TILE, body, 0, unroll=4)

    def panel(section, base, send_ref):
        def body(r, carry):
            features = lax.dot_general(
                weight_buf[section, pl.ds(base, 2 * HIDDEN)],
                normed_buf[r],
                (((1,), (1,)), ((), ())),
                preferred_element_type=jnp.float32,
            )
            features = features + bias_buf[section, pl.ds(base, 2 * HIDDEN)]
            mask = col_mask * row_mask_ref[row * TILE + r].astype(jnp.float32)
            values = mask * sigmoid(features[:HIDDEN]) * features[HIDDEN:]
            wide_buf[pl.ds(r, HIDDEN, stride=TILE), :] = values
            return carry

        lax.fori_loop(0, TILE, body, 0, unroll=4)

        def pack(i, carry):
            part = wide_buf[pl.ds(i * 16 * TILE, 16 * TILE), :]
            send_ref[pl.ds(i * 16, 16)] = part.reshape(16, TILE, LANE).astype(jnp.bfloat16)
            return carry

        lax.fori_loop(0, 8, pack, 0)

    def gate(section):
        def body(r, carry):
            values = jnp.dot(
                normed_buf[r], gate_weight_ref[section], preferred_element_type=jnp.float32
            )
            gate_buf[r] = sigmoid(values + gate_bias_ref[pl.ds(section, 1), :])
            return carry

        lax.fori_loop(0, TILE, body, 0, unroll=4)

    def finish(section):
        got = xrecv.at[section]

        def total(i, carry):
            return carry + jnp.sum(got[pl.ds(i * 16, 16)].astype(jnp.float32), axis=0)

        zero = jnp.zeros((TILE, LANE), jnp.float32)
        center = lax.fori_loop(0, 8, total, zero) * (1.0 / HIDDEN)

        def squares(i, carry):
            offset = got[pl.ds(i * 16, 16)].astype(jnp.float32) - center
            return carry + jnp.sum(offset * offset, axis=0)

        spread = lax.fori_loop(0, 8, squares, zero) * (1.0 / HIDDEN)
        scale = lax.rsqrt(spread + HIDDEN_EPSILON)

        def rescale(h, carry):
            offset = got[h].astype(jnp.float32) - center
            values = offset * scale * hidden_gain_ref[section, h] + hidden_shift_ref[section, h]
            wide_buf[pl.ds(pl.multiple_of(h * TILE, TILE), TILE), :] = values
            return carry

        lax.fori_loop(0, HIDDEN, rescale, 0, unroll=8)

        def body(r, carry):
            normed = wide_buf[pl.ds(r, HIDDEN, stride=TILE), :].astype(jnp.bfloat16)
            projected = lax.dot_general(
                normed,
                output_weight_ref[section],
                (((0,), (0,)), ((), ())),
                preferred_element_type=jnp.float32,
            )
            projected = projected + output_bias_ref[pl.ds(section, 1), :]
            pair_buf[r] = pair_buf[r] + gate_buf[r] * projected
            return carry

        for part in range(4):
            lax.fori_loop(part * 4, part * 4 + 4, body, 0, unroll=4)
            if section == 1:
                store(part).start()

    def store(part):
        some = pl.ds(part * 4, 4)
        return pltpu.make_async_copy(pair_buf.at[some], out_ref.at[some], io_sem.at[1 + part])

    def remote(src, dst, sent, got, there):
        return pltpu.make_async_remote_copy(
            src_ref=src,
            dst_ref=dst,
            send_sem=send_sem.at[sent],
            recv_sem=recv_sem.at[got],
            device_id=there,
            device_id_type=MESH,
        )

    def first(src, dst, sent, got, there, to_self):
        local = pltpu.make_async_copy(src, dst, recv_sem.at[got])
        if to_self is None:
            local.start()
        else:
            pl.when(to_self)(local.start)
            pl.when(jnp.logical_not(to_self))(remote(src, dst, sent, got, there).start)

    def got_all(got):
        pltpu.make_async_copy(left_send, left_send, recv_sem.at[got]).wait()

    def sent_all(sent):
        pltpu.make_async_copy(left_send, left_send, send_sem.at[sent]).wait()

    def sent_rest(sent, to_self):
        rest = left_send.at[pl.ds(0, HIDDEN - 1)]
        pltpu.make_async_copy(rest, rest, send_sem.at[sent]).wait()
        if to_self is not None:
            one = left_send.at[0]
            pl.when(jnp.logical_not(to_self))(
                pltpu.make_async_copy(one, one, send_sem.at[sent + 1]).wait
            )

    def target(t, to_half, to_core):
        dz, dy, dx = shuffled(t)
        z_t, y_t, hx_t = (z + dz) % 8, (y + dy) % 8, (hx + dx) % 2
        x_t = hx_t + to_half * (3 - 2 * hx_t)
        there = {"row": z_t * 8 + (y_t % 2) * 4 + x_t, "ch": (y_t // 2) * 2 + to_core}
        return z_t * 16 + y_t * 2 + hx_t, there

    def panel_sends(ref, slot, to_half, to_core, sent, gots, to_self):
        h_0, there_0 = target(0, to_half, to_core)
        first(ref.at[h_0], slot, sent + 1, gots[0], there_0, to_self)

        def sends(got):
            def body(t, carry):
                h_t, there = target(t, to_half, to_core)
                remote(ref.at[h_t], slot, sent, got, there).start()
                return carry

            return body

        lax.fori_loop(1, 64, sends(gots[0]), 0)
        lax.fori_loop(64, HIDDEN, sends(gots[1]), 0)

    partner = {"row": row + 3 - 2 * x, "ch": ch}
    sibling = {"row": row, "ch": ch + 1 - 2 * core}

    def update(section):
        pair_panel = pair_bufs.at[section]
        core_panel = core_bufs.at[section]
        s, g = 8 * section, 6 * section
        rows, lanes = pl.ds(x_lo * TILE, TILE), pl.ds(y_hi * LANE, LANE)
        if section == 0:
            pair_base, core_base = 2 * HIDDEN, 0
            pair_slot = pair_panel.at[core, z // 2, y_lo, x_hi, rows, lanes]
            core_slot = core_panel.at[core, pl.ds((z * 4 + y_lo * 2 + x_lo) * TILE, TILE), lanes]
            pair_to, core_to = (x_hi, z % 2), (x_hi, core)
            pair_self, core_self, x_self = core == z % 2, None, None
        else:
            pair_base, core_base = 0, 2 * HIDDEN
            block = pl.ds(((y_hi % 2) * 2 + core) * LANE, LANE)
            pair_slot = pair_panel.at[z // 4, z % 4, y_lo, x_hi, rows, block]
            core_slot = core_panel.at[z // 4, pl.ds((row % 32) * TILE, TILE), lanes]
            pair_to, core_to = (x_hi, y_hi // 2), (core, z // 4)
            pair_self = core == y_hi // 2
            core_self = x_self = jnp.logical_and(core == z // 4, core == x_hi)

        normalize(section)
        if section == 0:
            pl.semaphore_wait(barrier, 46)
            signals(ready_sem, plane, 32)
        panel(section, pair_base, right_send)
        if section == 0:
            pl.semaphore_wait(ready_sem, 31)
        panel_sends(right_send, pair_slot, *pair_to, s, (g, g + 1), pair_self)
        panel(section, core_base, left_send)
        panel_sends(left_send, core_slot, *core_to, s + 2, (g + 2, g + 2), core_self)
        gate(section)

        for dx in range(2):
            tiles = left_send.at[pl.ds(0, HIDDEN // 2)]
            pltpu.make_async_copy(tiles, tiles, recv_sem.at[g + dx]).wait()
            hx_s = (hx + dx) % 2
            from_rows = pl.ds((hx_s + half * (1 - 2 * hx_s)) * TILE, TILE)
            for outer in range(2):
                for inner in range(4):
                    for low in range(2):
                        block = pair_panel.at[outer, inner, low, half, from_rows]
                        remote(block, block, s + 4, g + 3, partner).start()
        got_all(g + 2)
        remote(core_panel.at[core], core_panel.at[core], s + 5, g + 4, sibling).start()
        got_all(g + 3)
        got_all(g + 4)

        if section == 0:
            products = None
            for part in range(2):
                term = lax.dot_general(
                    core_bufs[section, part],
                    pair_bufs[section, part].reshape(512, 512),
                    (((1,), (1,)), ((), ())),
                    preferred_element_type=jnp.float32,
                )
                products = term if products is None else products + term
        else:
            products = lax.dot_general(
                pair_bufs[section].reshape(1024, 512),
                core_bufs[section].reshape(1024, 512),
                (((0,), (0,)), ((), ())),
                preferred_element_type=jnp.float32,
            )
        xbuf[section] = products.astype(jnp.bfloat16)

        def cell(t):
            dz, dy, dx = shuffled(t)
            y_t = (y + dy) % 8
            if section == 0:
                z_t, low_t = (z + dz) % 8, (x_lo + dx) % 2
                block = z_t * 4 + (y_t % 2) * 2 + low_t
                row_t = z_t * 8 + (y_t % 2) * 4 + half * 2 + low_t
                core_t = core
            else:
                q_t = (z + dz % 4) % 4
                x_t = (x + (dz // 4) * 2 + dx) % 4
                block = q_t * 8 + (y_t % 2) * 4 + x_t
                row_t = core * 32 + block
                core_t = half
            src = xbuf.at[section, pl.ds(block * TILE, TILE), pl.ds((y_t // 2) * LANE, LANE)]
            return src, {"row": row_t, "ch": (y_t // 2) * 2 + core_t}

        x_slot = xrecv.at[section, own_h]
        src_0, there_0 = cell(0)
        first(src_0, x_slot, s + 7, g + 5, there_0, x_self)

        def body(t, carry):
            src, there = cell(t)
            remote(src, x_slot, s + 6, g + 5, there).start()
            return carry

        lax.fori_loop(1, HIDDEN, body, 0)
        sent_rest(s, pair_self)
        sent_rest(s + 2, core_self)
        sent_all(s + 4)
        sent_all(s + 5)
        got_all(g + 5)
        finish(section)
        sent_rest(s + 6, x_self)

    prepare(0)
    prepare(1)
    load.wait()
    update(0)
    update(1)
    for part in range(4):
        store(part).wait()


def local(
    pair_rep,
    residue_mask,
    pair_gain,
    pair_shift,
    panel_weight,
    panel_bias,
    gate_weight,
    gate_bias,
    hidden_gain,
    hidden_shift,
    output_weight,
    output_bias,
):
    smem = pl.BlockSpec(memory_space=pltpu.SMEM)
    vmem = pl.BlockSpec(memory_space=pltpu.VMEM)
    half = jnp.bfloat16
    return pl.pallas_call(
        evoformer_kernel,
        out_shape=jax.ShapeDtypeStruct(pair_rep.shape, jnp.float32),
        in_specs=[smem] * 3 + [pl.BlockSpec(memory_space=pl.ANY)] + [vmem] * 9,
        out_specs=pl.BlockSpec(memory_space=pl.ANY),
        scratch_shapes=[
            pltpu.VMEM((TILE, LANE, LANE), jnp.float32),
            pltpu.VMEM((2, 4 * HIDDEN, LANE), half),
            pltpu.VMEM((2, 4 * HIDDEN, LANE), jnp.float32),
            pltpu.VMEM((TILE, LANE, LANE), half),
            pltpu.VMEM((TILE, LANE, LANE), jnp.float32),
            pltpu.VMEM((HIDDEN * TILE, LANE), jnp.float32),
            pltpu.VMEM((HIDDEN, TILE, LANE), half),
            pltpu.VMEM((HIDDEN, TILE, LANE), half),
            pltpu.VMEM((2, 2, 4, 2, 2, 32, 512), half),
            pltpu.VMEM((2, 2, 512, 512), half),
            pltpu.VMEM((2, 512, 512), half),
            pltpu.VMEM((2, HIDDEN, TILE, LANE), half),
            pltpu.SemaphoreType.DMA((16,)),
            pltpu.SemaphoreType.DMA((12,)),
            pltpu.SemaphoreType.DMA((5,)),
            pltpu.SemaphoreType.REGULAR,
        ],
        compiler_params=pltpu.CompilerParams(collective_id=0, has_side_effects=True),
        name="evoformer",
    )(
        residue_mask,
        hidden_gain,
        hidden_shift,
        pair_rep,
        residue_mask.reshape(CHANNELS, LANE),
        pair_gain,
        pair_shift,
        panel_weight,
        panel_bias,
        gate_weight,
        gate_bias,
        output_weight,
        output_bias,
    )


def solution(mesh):
    return jax.shard_map(
        local,
        mesh=mesh,
        in_specs=(P("row", "ch", None), P(), P(), P(), P(), P(), P(), P(), P(), P(), P(), P()),
        out_specs=P("row", "ch", None),
        check_vma=False,
    )
```

```python
import functools

import jax
import jax.numpy as jnp
from jax import lax
from jax.experimental import pallas as pl
from jax.experimental.pallas import tpu as pltpu
from jax.sharding import PartitionSpec as P

PAIR_EPSILON = 1e-05
HIDDEN_EPSILON = 1.0
MESH = pl.DeviceIdType.MESH
HIDDEN = 128
TILE = 16
LANE = 128
CHANNELS = 8


def sigmoid(values):
    return 0.5 * jnp.tanh(0.5 * values) + 0.5


def span(offset, size):
    return min(offset, size - offset)


PANEL_WALK = sorted(
    ((dz, dy, dx) for dz in range(8) for dy in range(8) for dx in range(2)),
    key=lambda o: (-span(o[0], 8) - span(o[1], 8), -o[2], (3 * o[0] + 5 * o[1]) % 8),
)
CELL_WALKS = (
    PANEL_WALK,
    sorted(
        ((dz, dy, dx) for dz in range(4) for dy in range(8) for dx in range(4)),
        key=lambda o: (-2 * span(o[0], 4) - span(o[1], 8) - span(o[2], 4), (3 * o[0] + 5 * o[1]) % 8),
    ),
)


def evoformer_kernel(*refs):
    sources, refs = refs[:13], refs[13:]
    out_ref, loaded, refs = refs[0], refs[1:14], refs[14:]
    (
        row_mask_ref,
        hidden_gain_ref,
        hidden_shift_ref,
        pair_buf,
        col_mask_ref,
        pair_gain_ref,
        pair_shift_ref,
        panel_weight_ref,
        panel_bias_ref,
        gate_weight_ref,
        gate_bias_ref,
        output_weight_ref,
        output_bias_ref,
    ) = loaded
    (
        weight_buf,
        bias_buf,
        normed_buf,
        gate_buf,
        wide_buf,
        left_send,
        right_send,
        pair_bufs,
        core_bufs,
        total_buf,
        xbuf,
        xrecv,
        send_sem,
        recv_sem,
        io_sem,
        ready_sem,
    ) = refs
    row = lax.axis_index("row")
    ch = lax.axis_index("ch")
    z, y_lo, x = row // 8, (row // 4) % 2, row % 4
    y_hi, core = ch // 2, ch % 2
    y = y_hi * 2 + y_lo
    x_hi, x_lo = x // 2, x % 2
    hx = x + x_hi * (3 - 2 * x)
    half = x_hi
    own_h = z * 16 + y * 2 + hx

    barrier = pltpu.get_barrier_semaphore()

    def column(t):
        spot = (y_lo * CHANNELS + ch + t) % 16
        return {"row": z * 8 + (spot // CHANNELS) * 4 + x, "ch": spot % CHANNELS}

    def plane(t):
        spot = (z * 4 + x + t) % 32
        return {"row": (spot // 4) * 8 + y_lo * 4 + spot % 4, "ch": ch}

    def signals(sem, group, count):
        def body(t, carry):
            pl.semaphore_signal(sem, inc=1, device_id=group(t), device_id_type=MESH)
            return carry

        lax.fori_loop(1, count, body, 0)

    signals(barrier, plane, 32)
    signals(barrier, column, 16)
    loads = [
        pltpu.make_async_copy(source, ref, io_sem.at[4 + i])
        for i, (source, ref) in enumerate(zip(sources, loaded))
    ]
    for load in loads:
        load.start()
    for load in loads:
        load.wait()

    col_mask = col_mask_ref[pl.ds(ch, 1), :].astype(jnp.float32)

    def prepare(section):
        weight = panel_weight_ref[section].astype(jnp.float32)
        weight_buf[section] = weight.T.astype(jnp.bfloat16)
        bias = panel_bias_ref[pl.ds(section, 1), :]
        bias_buf[section] = jnp.broadcast_to(bias, (LANE, 4 * HIDDEN)).T

    def normalize(section):
        gain = pair_gain_ref[pl.ds(section, 1), :]
        shift = pair_shift_ref[pl.ds(section, 1), :]

        def body(r, carry):
            values = pair_buf[r]
            offset = values - jnp.mean(values, axis=-1, keepdims=True)
            spread = jnp.mean(offset * offset, axis=-1, keepdims=True)
            normed = offset * lax.rsqrt(spread + PAIR_EPSILON) * gain + shift
            normed_buf[r] = normed.astype(jnp.bfloat16)
            return carry

        lax.fori_loop(0, TILE, body, 0, unroll=4)

    def panel(section, base, send_ref):
        def body(r, carry):
            features = lax.dot_general(
                weight_buf[section, pl.ds(base, 2 * HIDDEN)],
                normed_buf[r],
                (((1,), (1,)), ((), ())),
                preferred_element_type=jnp.float32,
            )
            features = features + bias_buf[section, pl.ds(base, 2 * HIDDEN)]
            mask = col_mask * row_mask_ref[row * TILE + r].astype(jnp.float32)
            values = mask * sigmoid(features[:HIDDEN]) * features[HIDDEN:]
            wide_buf[pl.ds(r, HIDDEN, stride=TILE), :] = values
            return carry

        lax.fori_loop(0, TILE, body, 0, unroll=4)

        def pack(i, carry):
            part = wide_buf[pl.ds(i * 16 * TILE, 16 * TILE), :]
            send_ref[pl.ds(i * 16, 16)] = part.reshape(16, TILE, LANE).astype(jnp.bfloat16)
            return carry

        lax.fori_loop(0, 8, pack, 0)

    def gate(section):
        def body(r, carry):
            values = jnp.dot(
                normed_buf[r], gate_weight_ref[section], preferred_element_type=jnp.float32
            )
            gate_buf[r] = sigmoid(values + gate_bias_ref[pl.ds(section, 1), :])
            return carry

        lax.fori_loop(0, TILE, body, 0, unroll=4)

    def finish(section):
        got = xrecv.at[section]

        def total(i, carry):
            return carry + jnp.sum(got[pl.ds(i * 16, 16)].astype(jnp.float32), axis=0)

        zero = jnp.zeros((TILE, LANE), jnp.float32)
        center = lax.fori_loop(0, 8, total, zero) * (1.0 / HIDDEN)

        def squares(i, carry):
            offset = got[pl.ds(i * 16, 16)].astype(jnp.float32) - center
            return carry + jnp.sum(offset * offset, axis=0)

        spread = lax.fori_loop(0, 8, squares, zero) * (1.0 / HIDDEN)
        scale = lax.rsqrt(spread + HIDDEN_EPSILON)

        def rescale(h, carry):
            offset = got[h].astype(jnp.float32) - center
            values = offset * scale * hidden_gain_ref[section, h] + hidden_shift_ref[section, h]
            wide_buf[pl.ds(pl.multiple_of(h * TILE, TILE), TILE), :] = values
            return carry

        lax.fori_loop(0, HIDDEN, rescale, 0, unroll=8)

        def body(r, carry):
            normed = wide_buf[pl.ds(r, HIDDEN, stride=TILE), :].astype(jnp.bfloat16)
            projected = lax.dot_general(
                normed,
                output_weight_ref[section],
                (((0,), (0,)), ((), ())),
                preferred_element_type=jnp.float32,
            )
            projected = projected + output_bias_ref[pl.ds(section, 1), :]
            pair_buf[r] = pair_buf[r] + gate_buf[r] * projected
            return carry

        for part in range(4):
            lax.fori_loop(part * 4, part * 4 + 4, body, 0, unroll=4)
            if section == 1:
                store(part).start()

    def store(part):
        some = pl.ds(part * 4, 4)
        return pltpu.make_async_copy(pair_buf.at[some], out_ref.at[some], io_sem.at[part])

    def remote(src, dst, sent, got, there):
        return pltpu.make_async_remote_copy(
            src_ref=src,
            dst_ref=dst,
            send_sem=send_sem.at[sent],
            recv_sem=recv_sem.at[got],
            device_id=there,
            device_id_type=MESH,
        )

    def first(src, dst, sent, got, there, to_self):
        local = pltpu.make_async_copy(src, dst, recv_sem.at[got])
        if to_self is None:
            local.start()
        else:
            pl.when(to_self)(local.start)
            pl.when(jnp.logical_not(to_self))(remote(src, dst, sent, got, there).start)

    def got_all(got):
        pltpu.make_async_copy(left_send, left_send, recv_sem.at[got]).wait()

    def sent_all(sent):
        pltpu.make_async_copy(left_send, left_send, send_sem.at[sent]).wait()

    def sent_rest(sent, to_self):
        rest = left_send.at[pl.ds(0, HIDDEN - 1)]
        pltpu.make_async_copy(rest, rest, send_sem.at[sent]).wait()
        if to_self is not None:
            one = left_send.at[0]
            pl.when(jnp.logical_not(to_self))(
                pltpu.make_async_copy(one, one, send_sem.at[sent + 1]).wait
            )

    zs = [(z + d) % 8 for d in range(8)]
    ys = [(y + d) % 8 for d in range(8)]
    y_rows = [(y_t % 2) * 4 for y_t in ys]
    y_chs = [(y_t // 2) * 2 for y_t in ys]

    def panel_sends(ref, slot, to_half, to_core, sent, gots, to_self, dxs):
        hs = [(hx + d) % 2 for d in range(2)]
        xs = [hx_t + to_half * (3 - 2 * hx_t) for hx_t in hs]
        for dz, dy, dx in PANEL_WALK:
            if dx not in dxs:
                continue
            src = ref.at[zs[dz] * 16 + ys[dy] * 2 + hs[dx]]
            there = {"row": zs[dz] * 8 + y_rows[dy] + xs[dx], "ch": y_chs[dy] + to_core}
            if (dz, dy, dx) == (0, 0, 0):
                first(src, slot, sent + 1, gots[0], there, to_self)
            else:
                remote(src, slot, sent, gots[dx], there).start()

    partner = {"row": row + 3 - 2 * x, "ch": ch}
    sibling = {"row": row, "ch": ch + 1 - 2 * core}

    def update(section):
        pair_panel = pair_bufs.at[section]
        core_panel = core_bufs.at[section]
        s, g = 8 * section, 6 * section
        rows, lanes = pl.ds(x_lo * TILE, TILE), pl.ds(y_hi * LANE, LANE)
        if section == 0:
            pair_base, core_base = 2 * HIDDEN, 0
            pair_slot = pair_panel.at[core, z // 2, y_lo, x_hi, rows, lanes]
            core_slot = core_panel.at[core, pl.ds((z * 4 + y_lo * 2 + x_lo) * TILE, TILE), lanes]
            pair_to, core_to = (x_hi, z % 2), (x_hi, core)
            pair_self, core_self, x_self = core == z % 2, None, None
        else:
            pair_base, core_base = 0, 2 * HIDDEN
            pair_slot = pair_panel.at[z // 4, z % 4, y_lo, x_hi, rows, lanes]
            core_slot = core_panel.at[z // 4, pl.ds((row % 32) * TILE, TILE), lanes]
            pair_to, core_to = (x_hi, core), (core, z // 4)
            pair_self = None
            core_self = jnp.logical_and(core == z // 4, core == x_hi)
            x_self = jnp.logical_and(core == z % 2, core == x_hi)

        normalize(section)
        if section == 0:
            pl.semaphore_wait(barrier, 46)
            signals(ready_sem, column, 16)
        panel(section, pair_base, right_send)
        if section == 0:
            pl.semaphore_wait(ready_sem, 15)
        panel_sends(right_send, pair_slot, *pair_to, s, (g, g + 1), pair_self, (1,))
        panel_sends(right_send, pair_slot, *pair_to, s, (g, g + 1), pair_self, (0,))
        panel(section, core_base, left_send)
        panel_sends(left_send, core_slot, *core_to, s + 2, (g + 2, g + 2), core_self, (0, 1))
        gate(section)

        for dx in (1, 0):
            tiles = left_send.at[pl.ds(0, HIDDEN // 2)]
            pltpu.make_async_copy(tiles, tiles, recv_sem.at[g + dx]).wait()
            hx_s = (hx + dx) % 2
            from_rows = pl.ds((hx_s + half * (1 - 2 * hx_s)) * TILE, TILE)
            for outer in range(2):
                for inner in range(4):
                    for low in range(2):
                        block = pair_panel.at[outer, inner, low, half, from_rows]
                        remote(block, block, s + 4, g + 3, partner).start()
        got_all(g + 2)
        remote(core_panel.at[core], core_panel.at[core], s + 5, g + 4, sibling).start()
        got_all(g + 3)

        def term(part):
            if section == 0:
                return lax.dot_general(
                    core_bufs[section, part],
                    pair_bufs[section, part].reshape(512, 512),
                    (((1,), (1,)), ((), ())),
                    preferred_element_type=jnp.float32,
                )
            return lax.dot_general(
                pair_bufs[section, part].reshape(512, 512),
                core_bufs[section, part],
                (((0,), (0,)), ((), ())),
                preferred_element_type=jnp.float32,
            )

        total_buf[...] = term(core)
        got_all(g + 4)
        xbuf[section] = (total_buf[...] + term(1 - core)).astype(jnp.bfloat16)

        x_slot = xrecv.at[section, own_h]
        odd = (z + core) % 2
        returns = zs if section == 0 else [(z + odd + 2 * d) % 8 for d in range(4)]
        lows = [(x_lo + d) % 2 for d in range(2)]
        xs = [half * 2 + low_t for low_t in lows] if section == 0 else [(x + d) % 4 for d in range(4)]
        for dz, dy, dx in CELL_WALKS[section]:
            z_t, x_t = returns[dz], xs[dx]
            if section == 0:
                block = z_t * 4 + (ys[dy] % 2) * 2 + lows[dx]
            else:
                block = (z_t // 2) * 8 + y_rows[dy] + x_t
            src = xbuf.at[section, pl.ds(block * TILE, TILE), pl.ds((ys[dy] // 2) * LANE, LANE)]
            there = {
                "row": z_t * 8 + y_rows[dy] + x_t,
                "ch": y_chs[dy] + (core if section == 0 else half),
            }
            if (dz, dy, dx) == (0, 0, 0):
                first(src, x_slot, s + 7, g + 5, there, x_self)
            else:
                remote(src, x_slot, s + 6, g + 5, there).start()
        sent_rest(s, pair_self)
        sent_rest(s + 2, core_self)
        sent_all(s + 4)
        sent_all(s + 5)
        got_all(g + 5)
        finish(section)
        sent_rest(s + 6, x_self)

    prepare(0)
    prepare(1)
    update(0)
    update(1)
    for part in range(4):
        store(part).wait()


def local(
    pair_rep,
    residue_mask,
    pair_gain,
    pair_shift,
    panel_weight,
    panel_bias,
    gate_weight,
    gate_bias,
    hidden_gain,
    hidden_shift,
    output_weight,
    output_bias,
):
    half = jnp.bfloat16
    operands = (
        residue_mask,
        hidden_gain,
        hidden_shift,
        pair_rep,
        residue_mask.reshape(CHANNELS, LANE),
        pair_gain,
        pair_shift,
        panel_weight,
        panel_bias,
        gate_weight,
        gate_bias,
        output_weight,
        output_bias,
    )
    return pl.pallas_call(
        evoformer_kernel,
        out_shape=jax.ShapeDtypeStruct(pair_rep.shape, jnp.float32),
        in_specs=[pl.BlockSpec(memory_space=pltpu.HBM)] * len(operands),
        out_specs=pl.BlockSpec(memory_space=pl.ANY),
        scratch_shapes=[
            *(
                (pltpu.SMEM if i < 3 else pltpu.VMEM)(operand.shape, operand.dtype)
                for i, operand in enumerate(operands)
            ),
            pltpu.VMEM((2, 4 * HIDDEN, LANE), half),
            pltpu.VMEM((2, 4 * HIDDEN, LANE), jnp.float32),
            pltpu.VMEM((TILE, LANE, LANE), half),
            pltpu.VMEM((TILE, LANE, LANE), jnp.float32),
            pltpu.VMEM((HIDDEN * TILE, LANE), jnp.float32),
            pltpu.VMEM((HIDDEN, TILE, LANE), half),
            pltpu.VMEM((HIDDEN, TILE, LANE), half),
            pltpu.VMEM((2, 2, 4, 2, 2, 32, 512), half),
            pltpu.VMEM((2, 2, 512, 512), half),
            pltpu.VMEM((512, 512), jnp.float32),
            pltpu.VMEM((2, 512, 512), half),
            pltpu.VMEM((2, HIDDEN, TILE, LANE), half),
            pltpu.SemaphoreType.DMA((16,)),
            pltpu.SemaphoreType.DMA((12,)),
            pltpu.SemaphoreType.DMA((4 + len(operands),)),
            pltpu.SemaphoreType.REGULAR,
        ],
        compiler_params=pltpu.CompilerParams(collective_id=0, has_side_effects=True),
        name="evoformer",
    )(*operands)


def solution(mesh):
    return jax.shard_map(
        local,
        mesh=mesh,
        in_specs=(P("row", "ch", None), P(), P(), P(), P(), P(), P(), P(), P(), P(), P(), P()),
        out_specs=P("row", "ch", None),
        check_vma=False,
    )
```

```python
import functools

import jax
import jax.numpy as jnp
from jax import lax
from jax.experimental import pallas as pl
from jax.experimental.pallas import tpu as pltpu
from jax.sharding import PartitionSpec as P

PAIR_EPSILON = 1e-05
HIDDEN_EPSILON = 1.0
MESH = pl.DeviceIdType.MESH
HIDDEN = 128
TILE = 16
LANE = 128
CHANNELS = 8


def sigmoid(values):
    return 0.5 * jnp.tanh(0.5 * values) + 0.5


def span(offset, size):
    return min(offset, size - offset)


PANEL_WALK = sorted(
    ((dz, dy, dx) for dz in range(8) for dy in range(8) for dx in range(2)),
    key=lambda o: (-span(o[0], 8) - span(o[1], 8), -o[2], (3 * o[0] + 5 * o[1]) % 8),
)
CELL_WALKS = (
    PANEL_WALK,
    sorted(
        ((dz, dy, dx) for dz in range(4) for dy in range(8) for dx in range(4)),
        key=lambda o: (-2 * span(o[0], 4) - span(o[1], 8) - span(o[2], 4), (3 * o[0] + 5 * o[1]) % 8),
    ),
)


def evoformer_kernel(*refs):
    sources, refs = refs[:13], refs[13:]
    out_ref, loaded, refs = refs[0], refs[1:14], refs[14:]
    (
        row_mask_ref,
        hidden_gain_ref,
        hidden_shift_ref,
        pair_buf,
        col_mask_ref,
        pair_gain_ref,
        pair_shift_ref,
        panel_weight_ref,
        panel_bias_ref,
        gate_weight_ref,
        gate_bias_ref,
        output_weight_ref,
        output_bias_ref,
    ) = loaded
    (
        weight_buf,
        bias_buf,
        normed_buf,
        gate_buf,
        wide_buf,
        left_send,
        right_send,
        pair_bufs,
        core_bufs,
        total_buf,
        xbuf,
        xrecv,
        send_sem,
        recv_sem,
        io_sem,
        ready_sem,
    ) = refs
    row = lax.axis_index("row")
    ch = lax.axis_index("ch")
    z, y_lo, x = row // 8, (row // 4) % 2, row % 4
    y_hi, core = ch // 2, ch % 2
    y = y_hi * 2 + y_lo
    x_hi, x_lo = x // 2, x % 2
    hx = x + x_hi * (3 - 2 * x)
    half = x_hi
    own_h = z * 16 + y * 2 + hx

    barrier = pltpu.get_barrier_semaphore()

    def signals(sem, spots):
        for there in spots:
            pl.semaphore_signal(sem, inc=1, device_id=there, device_id_type=MESH)

    plane = [
        {"row": ((z + dz) % 8) * 8 + y_lo * 4 + (x + dx) % 4, "ch": ch}
        for dz, dx in sorted(
            ((dz, dx) for dz in range(8) for dx in range(4)),
            key=lambda o: -span(o[0], 8) - span(o[1], 4),
        )[:-1]
    ]
    column = [
        {"row": z * 8 + ((y_lo + dl) % 2) * 4 + x, "ch": (ch + dc) % CHANNELS}
        for dc, dl in sorted(
            ((dc, dl) for dc in range(8) for dl in range(2)),
            key=lambda o: -span(o[0], 8) - o[1],
        )[:-1]
    ]
    signals(barrier, plane)
    signals(barrier, column)
    loads = [
        pltpu.make_async_copy(source, ref, io_sem.at[4 + i])
        for i, (source, ref) in enumerate(zip(sources, loaded))
    ]
    for load in loads:
        load.start()
    for load in loads:
        load.wait()

    col_mask = col_mask_ref[pl.ds(ch, 1), :].astype(jnp.float32)

    def prepare(section):
        weight = panel_weight_ref[section].astype(jnp.float32)
        weight_buf[section] = weight.T.astype(jnp.bfloat16)
        bias = panel_bias_ref[pl.ds(section, 1), :]
        bias_buf[section] = jnp.broadcast_to(bias, (LANE, 4 * HIDDEN)).T

    def normalize(section):
        gain = pair_gain_ref[pl.ds(section, 1), :]
        shift = pair_shift_ref[pl.ds(section, 1), :]

        def body(r, carry):
            values = pair_buf[r]
            offset = values - jnp.mean(values, axis=-1, keepdims=True)
            spread = jnp.mean(offset * offset, axis=-1, keepdims=True)
            normed = offset * lax.rsqrt(spread + PAIR_EPSILON) * gain + shift
            normed_buf[r] = normed.astype(jnp.bfloat16)
            return carry

        lax.fori_loop(0, TILE, body, 0, unroll=4)

    def panel(section, base, send_ref):
        def body(r, carry):
            features = lax.dot_general(
                weight_buf[section, pl.ds(base, 2 * HIDDEN)],
                normed_buf[r],
                (((1,), (1,)), ((), ())),
                preferred_element_type=jnp.float32,
            )
            features = features + bias_buf[section, pl.ds(base, 2 * HIDDEN)]
            mask = col_mask * row_mask_ref[row * TILE + r].astype(jnp.float32)
            values = mask * sigmoid(features[:HIDDEN]) * features[HIDDEN:]
            wide_buf[pl.ds(r, HIDDEN, stride=TILE), :] = values
            return carry

        lax.fori_loop(0, TILE, body, 0, unroll=4)

        def pack(i, carry):
            part = wide_buf[pl.ds(i * 16 * TILE, 16 * TILE), :]
            send_ref[pl.ds(i * 16, 16)] = part.reshape(16, TILE, LANE).astype(jnp.bfloat16)
            return carry

        lax.fori_loop(0, 8, pack, 0)

    def gate(section):
        def body(r, carry):
            values = jnp.dot(
                normed_buf[r], gate_weight_ref[section], preferred_element_type=jnp.float32
            )
            gate_buf[r] = sigmoid(values + gate_bias_ref[pl.ds(section, 1), :])
            return carry

        lax.fori_loop(0, TILE, body, 0, unroll=4)

    def finish(section):
        got = xrecv.at[section]

        def total(i, carry):
            return carry + jnp.sum(got[pl.ds(i * 16, 16)].astype(jnp.float32), axis=0)

        zero = jnp.zeros((TILE, LANE), jnp.float32)
        center = lax.fori_loop(0, 8, total, zero) * (1.0 / HIDDEN)

        def squares(i, carry):
            offset = got[pl.ds(i * 16, 16)].astype(jnp.float32) - center
            return carry + jnp.sum(offset * offset, axis=0)

        spread = lax.fori_loop(0, 8, squares, zero) * (1.0 / HIDDEN)
        scale = lax.rsqrt(spread + HIDDEN_EPSILON)

        def rescale(h, carry):
            offset = got[h].astype(jnp.float32) - center
            values = offset * scale * hidden_gain_ref[section, h] + hidden_shift_ref[section, h]
            wide_buf[pl.ds(pl.multiple_of(h * TILE, TILE), TILE), :] = values
            return carry

        lax.fori_loop(0, HIDDEN, rescale, 0, unroll=8)

        def body(r, carry):
            normed = wide_buf[pl.ds(r, HIDDEN, stride=TILE), :].astype(jnp.bfloat16)
            projected = lax.dot_general(
                normed,
                output_weight_ref[section],
                (((0,), (0,)), ((), ())),
                preferred_element_type=jnp.float32,
            )
            projected = projected + output_bias_ref[pl.ds(section, 1), :]
            pair_buf[r] = pair_buf[r] + gate_buf[r] * projected
            return carry

        for part in range(4):
            lax.fori_loop(part * 4, part * 4 + 4, body, 0, unroll=4)
            if section == 1:
                store(part).start()

    def store(part):
        some = pl.ds(part * 4, 4)
        return pltpu.make_async_copy(pair_buf.at[some], out_ref.at[some], io_sem.at[part])

    def remote(src, dst, sent, got, there):
        return pltpu.make_async_remote_copy(
            src_ref=src,
            dst_ref=dst,
            send_sem=send_sem.at[sent],
            recv_sem=recv_sem.at[got],
            device_id=there,
            device_id_type=MESH,
        )

    def first(src, dst, sent, got, there, to_self):
        local = pltpu.make_async_copy(src, dst, recv_sem.at[got])
        if to_self is None:
            local.start()
        else:
            pl.when(to_self)(local.start)
            pl.when(jnp.logical_not(to_self))(remote(src, dst, sent, got, there).start)

    def got_all(got):
        pltpu.make_async_copy(left_send, left_send, recv_sem.at[got]).wait()

    def sent_all(sent):
        pltpu.make_async_copy(left_send, left_send, send_sem.at[sent]).wait()

    def sent_rest(sent, to_self):
        rest = left_send.at[pl.ds(0, HIDDEN - 1)]
        pltpu.make_async_copy(rest, rest, send_sem.at[sent]).wait()
        if to_self is not None:
            one = left_send.at[0]
            pl.when(jnp.logical_not(to_self))(
                pltpu.make_async_copy(one, one, send_sem.at[sent + 1]).wait
            )

    zs = [(z + d) % 8 for d in range(8)]
    ys = [(y + d) % 8 for d in range(8)]
    y_rows = [(y_t % 2) * 4 for y_t in ys]
    y_chs = [(y_t // 2) * 2 for y_t in ys]

    def panel_sends(ref, slot, to_half, to_core, sent, gots, to_self, dxs):
        hs = [(hx + d) % 2 for d in range(2)]
        xs = [hx_t + to_half * (3 - 2 * hx_t) for hx_t in hs]
        for dz, dy, dx in PANEL_WALK:
            if dx not in dxs:
                continue
            src = ref.at[zs[dz] * 16 + ys[dy] * 2 + hs[dx]]
            there = {"row": zs[dz] * 8 + y_rows[dy] + xs[dx], "ch": y_chs[dy] + to_core}
            if (dz, dy, dx) == (0, 0, 0):
                first(src, slot, sent + 1, gots[0], there, to_self)
            else:
                remote(src, slot, sent, gots[dx], there).start()

    partner = {"row": row + 3 - 2 * x, "ch": ch}
    sibling = {"row": row, "ch": ch + 1 - 2 * core}

    def update(section):
        pair_panel = pair_bufs.at[section]
        core_panel = core_bufs.at[section]
        s, g = 8 * section, 6 * section
        rows, lanes = pl.ds(x_lo * TILE, TILE), pl.ds(y_hi * LANE, LANE)
        if section == 0:
            pair_base, core_base = 2 * HIDDEN, 0
            pair_slot = pair_panel.at[core, z // 2, y_lo, x_hi, rows, lanes]
            core_slot = core_panel.at[core, pl.ds((z * 4 + y_lo * 2 + x_lo) * TILE, TILE), lanes]
            pair_to, core_to = (x_hi, z % 2), (x_hi, core)
            pair_self, core_self, x_self = core == z % 2, None, None
        else:
            pair_base, core_base = 0, 2 * HIDDEN
            pair_slot = pair_panel.at[z // 4, z % 4, y_lo, x_hi, rows, lanes]
            core_slot = core_panel.at[z // 4, pl.ds((row % 32) * TILE, TILE), lanes]
            pair_to, core_to = (x_hi, core), (core, z // 4)
            pair_self = None
            core_self = jnp.logical_and(core == z // 4, core == x_hi)
            x_self = jnp.logical_and(core == z % 2, core == x_hi)

        normalize(section)
        if section == 0:
            pl.semaphore_wait(barrier, 46)
            signals(ready_sem, column)
        panel(section, pair_base, right_send)
        if section == 0:
            pl.semaphore_wait(ready_sem, 15)
        panel_sends(right_send, pair_slot, *pair_to, s, (g, g + 1), pair_self, (1,))
        panel_sends(right_send, pair_slot, *pair_to, s, (g, g + 1), pair_self, (0,))
        panel(section, core_base, left_send)
        panel_sends(left_send, core_slot, *core_to, s + 2, (g + 2, g + 2), core_self, (0, 1))
        gate(section)

        for dx in (1, 0):
            tiles = left_send.at[pl.ds(0, HIDDEN // 2)]
            pltpu.make_async_copy(tiles, tiles, recv_sem.at[g + dx]).wait()
            hx_s = (hx + dx) % 2
            from_rows = pl.ds((hx_s + half * (1 - 2 * hx_s)) * TILE, TILE)
            for outer in range(2):
                for inner in range(4):
                    for low in range(2):
                        block = pair_panel.at[outer, inner, low, half, from_rows]
                        remote(block, block, s + 4, g + 3, partner).start()
        got_all(g + 2)
        remote(core_panel.at[core], core_panel.at[core], s + 5, g + 4, sibling).start()
        got_all(g + 3)

        def term(part):
            if section == 0:
                return lax.dot_general(
                    core_bufs[section, part],
                    pair_bufs[section, part].reshape(512, 512),
                    (((1,), (1,)), ((), ())),
                    preferred_element_type=jnp.float32,
                )
            return lax.dot_general(
                pair_bufs[section, part].reshape(512, 512),
                core_bufs[section, part],
                (((0,), (0,)), ((), ())),
                preferred_element_type=jnp.float32,
            )

        total_buf[...] = term(core)
        got_all(g + 4)
        xbuf[section] = (total_buf[...] + term(1 - core)).astype(jnp.bfloat16)

        x_slot = xrecv.at[section, own_h]
        odd = (z + core) % 2
        returns = zs if section == 0 else [(z + odd + 2 * d) % 8 for d in range(4)]
        lows = [(x_lo + d) % 2 for d in range(2)]
        xs = [half * 2 + low_t for low_t in lows] if section == 0 else [(x + d) % 4 for d in range(4)]
        for dz, dy, dx in CELL_WALKS[section]:
            z_t, x_t = returns[dz], xs[dx]
            if section == 0:
                block = z_t * 4 + (ys[dy] % 2) * 2 + lows[dx]
            else:
                block = (z_t // 2) * 8 + y_rows[dy] + x_t
            src = xbuf.at[section, pl.ds(block * TILE, TILE), pl.ds((ys[dy] // 2) * LANE, LANE)]
            there = {
                "row": z_t * 8 + y_rows[dy] + x_t,
                "ch": y_chs[dy] + (core if section == 0 else half),
            }
            if (dz, dy, dx) == (0, 0, 0):
                first(src, x_slot, s + 7, g + 5, there, x_self)
            else:
                remote(src, x_slot, s + 6, g + 5, there).start()
        sent_rest(s, pair_self)
        sent_rest(s + 2, core_self)
        sent_all(s + 4)
        sent_all(s + 5)
        got_all(g + 5)
        finish(section)
        sent_rest(s + 6, x_self)

    prepare(0)
    prepare(1)
    update(0)
    update(1)
    for part in range(4):
        store(part).wait()


def local(
    pair_rep,
    residue_mask,
    pair_gain,
    pair_shift,
    panel_weight,
    panel_bias,
    gate_weight,
    gate_bias,
    hidden_gain,
    hidden_shift,
    output_weight,
    output_bias,
):
    half = jnp.bfloat16
    operands = (
        residue_mask,
        hidden_gain,
        hidden_shift,
        pair_rep,
        residue_mask.reshape(CHANNELS, LANE),
        pair_gain,
        pair_shift,
        panel_weight,
        panel_bias,
        gate_weight,
        gate_bias,
        output_weight,
        output_bias,
    )
    return pl.pallas_call(
        evoformer_kernel,
        out_shape=jax.ShapeDtypeStruct(pair_rep.shape, jnp.float32),
        in_specs=[pl.BlockSpec(memory_space=pltpu.HBM)] * len(operands),
        out_specs=pl.BlockSpec(memory_space=pl.ANY),
        scratch_shapes=[
            *(
                (pltpu.SMEM if i < 3 else pltpu.VMEM)(operand.shape, operand.dtype)
                for i, operand in enumerate(operands)
            ),
            pltpu.VMEM((2, 4 * HIDDEN, LANE), half),
            pltpu.VMEM((2, 4 * HIDDEN, LANE), jnp.float32),
            pltpu.VMEM((TILE, LANE, LANE), half),
            pltpu.VMEM((TILE, LANE, LANE), jnp.float32),
            pltpu.VMEM((HIDDEN * TILE, LANE), jnp.float32),
            pltpu.VMEM((HIDDEN, TILE, LANE), half),
            pltpu.VMEM((HIDDEN, TILE, LANE), half),
            pltpu.VMEM((2, 2, 4, 2, 2, 32, 512), half),
            pltpu.VMEM((2, 2, 512, 512), half),
            pltpu.VMEM((512, 512), jnp.float32),
            pltpu.VMEM((2, 512, 512), half),
            pltpu.VMEM((2, HIDDEN, TILE, LANE), half),
            pltpu.SemaphoreType.DMA((16,)),
            pltpu.SemaphoreType.DMA((12,)),
            pltpu.SemaphoreType.DMA((4 + len(operands),)),
            pltpu.SemaphoreType.REGULAR,
        ],
        compiler_params=pltpu.CompilerParams(collective_id=0, has_side_effects=True),
        name="evoformer",
    )(*operands)


def solution(mesh):
    return jax.shard_map(
        local,
        mesh=mesh,
        in_specs=(P("row", "ch", None), P(), P(), P(), P(), P(), P(), P(), P(), P(), P(), P()),
        out_specs=P("row", "ch", None),
        check_vma=False,
    )
```
